256 devices in a mesh: rep: 4 (over z_hi), exp: 64 (over z_lo, x, y, core).
Axes of the slice: x: 4, y: 4, z: 8 (z_hi: 4, z_lo: 2; z = z_hi * 2 + z_lo), core: 2. Of those that a mesh axis runs over, the one named last changes fastest.
Arguments:
- act_a: bfloat16 [32768, 3584], P(('rep', 'exp')), may hold values from -6 to 6
- grad_a: bfloat16 [32768, 2, 1024], P(('rep', 'exp')), may hold values from -0.125 to 0.125
- route_a: int32 [32768, 2], P(('rep', 'exp')), may hold values from 0 to 63, all different within a row; in each aligned block of 128 rows (0 to 127, 128 to 255, ...) at most 5 rows name the same one
- act_b: bfloat16 [32768, 3584], P(('rep', 'exp')), may hold values from -6 to 6
- grad_b: bfloat16 [32768, 2, 1024], P(('rep', 'exp')), may hold values from -0.125 to 0.125
- route_b: int32 [32768, 2], P(('rep', 'exp')), may hold values from 0 to 31, all different within a row; in each aligned block of 128 rows (0 to 127, 128 to 255, ...) at most 10 rows name the same one
Outputs:
- wgrad_a: bfloat16 [64, 3584, 1024], P('exp', 'rep')
- wgrad_b: bfloat16 [64, 1792, 1024], P('exp', 'rep')
The draws below stay inside these ranges and needn't reach their ends.
Inputs may be any that keep to these rules, and one draw needn't show every extreme that they name: `route_a`: each token names 2 different experts of layer A; the 128 tokens of one device name any one expert at most 5 times. `route_b`: each token names 2 different experts of layer B; the 128 tokens of one device name any one expert at most 2 * 5 times.
All inputs are finite; a program needn't handle non-finite values.
Results may differ from the reference program's by a relative error of at most 0.013.
Values may be sent and summed in bfloat16 or wider, within the bound.
No kernel may reach another device: no remote copies, remote signals or barrier semaphores. Data moves between devices by JAX's collectives and lax.ppermute only.
A program may use at most 128 MiB of HBM per device.

```python
import math
import jax
import jax.numpy as jnp
import numpy as np
from jax import lax

DW = 3584
FW = 1024
TOK_DEV = 128
TOP = 2
MOST = 5
EXP_A = 64
EXP_B = 32
TOKENS = 32768
N_REP = 4
N_EXP = 64
DEVICES = 256


def block_levels(own_key, extent, split, smallest, high):
    factor_of, own = 1.0, jax.random.fold_in(own_key, 6)
    for axis_at, blocks in split:
        draws = jnp.exp(jax.random.uniform(jax.random.fold_in(own, axis_at), (blocks,), jnp.float32, smallest / len(split), high / len(split)))
        factor_of = factor_of * jnp.repeat(draws, extent[axis_at] // blocks).reshape([-1 if axis == axis_at else 1 for axis in range(len(extent))])
    return factor_of


def routed_block(key, own, number, rows, count, top, reach, lean):
    ranking = jax.random.permutation(key, count)
    crowded, usual = load_shares(count, rows * top, reach, lean, True), load_shares(count, rows * top, reach, lean, False)
    places = jnp.arange(count)

    def named(lengths, offset_by):
        used = int((lengths > 0).sum())
        fixed = max(1, used // 4)
        shifted = fixed + (places - fixed + offset_by * (used - fixed)) % max(1, count - fixed)
        return jnp.zeros((count,), jnp.int32).at[ranking[jnp.where(places < fixed, places, shifted)]].set(jnp.asarray(lengths, jnp.int32))

    lengths = jnp.where(number % 4 == 0, named(crowded, number // 4), named(usual, number - number // 4 - 1))
    mixed = jax.random.permutation(jax.random.fold_in(own, 3), count)
    source_of, receiver = mixed[0:count // 2 * 2:2], mixed[1:count // 2 * 2:2]
    room = jnp.minimum(lengths[source_of] - 1, reach - lengths[receiver]) // 2
    room = jnp.where((source_of == ranking[0]) | (receiver == ranking[0]) | (lengths[receiver] == 0), 0, jnp.maximum(room, 0))
    shifted = jax.random.randint(jax.random.fold_in(own, 4), (count // 2,), 0, 1 << 20) % (room + 1)
    lengths = lengths.at[source_of].add(-shifted).at[receiver].add(shifted)
    members = jnp.searchsorted(jnp.cumsum(lengths), jnp.arange(rows * top), side="right").astype(jnp.int32)
    table = members.reshape(top, rows).T
    table = table[jax.random.permutation(jax.random.fold_in(own, 1), rows)]
    offset_by = jax.random.randint(jax.random.fold_in(own, 2), (rows, 1), 0, top)
    return jnp.take_along_axis(table, (jnp.arange(top)[None, :] + offset_by) % top, axis=1)


def load_shares(number_of, total, limit, slope, full):
    weights = [(1 << 20) // math.isqrt(standing ** slope) + 1 for standing in range(1, number_of + 1)]
    largest = limit if full else min(limit, max(-(-total // number_of), total * weights[0] // sum(weights)))
    least = 1 if total - largest >= number_of - 1 else 0
    given, rest = [largest] + [least] * (number_of - 1), total - largest - least * (number_of - 1)
    while rest > 0:
        movable = [i for i in range(1, number_of) if given[i] < largest] or [i for i in range(1, number_of) if given[i] < limit]
        mass, remaining = sum([weights[i] for i in movable]), rest
        for i in movable:
            extra = min(limit - given[i], max(1, remaining * weights[i] // mass), rest)
            given[i] = given[i] + extra
            rest = rest - extra
    return np.array(given)


def gaussian(stream_key, extent, scale, limit, pieces=(), kind=jnp.bfloat16):
    result = jax.random.normal(stream_key, extent, jnp.float32) * scale
    if len(pieces) > 0:
        result = block_levels(stream_key, extent, pieces, -0.22, 0.18) * result
    return jnp.clip(result, min=-limit, max=limit).astype(kind)


def setup_inputs(seed: int = 0) -> dict:
    splits = jax.random.split(jax.random.key(seed), 7)
    act_a = gaussian(splits[0], (TOKENS, DW), 1.0, 6.0, ((0, 256),))
    grad_a = gaussian(splits[1], (TOKENS, TOP, FW), 0.02, 0.125, ((0, 256),))
    route_a_keys = jax.random.split(jax.random.fold_in(splits[2], 1), TOKENS // TOK_DEV)
    route_a_turns = jax.random.permutation(jax.random.fold_in(splits[2], 3), TOKENS // TOK_DEV)
    route_a = jax.vmap(lambda own, number: routed_block(jax.random.fold_in(splits[2], 2), own, number, TOK_DEV, EXP_A, TOP, MOST, 2))(route_a_keys, route_a_turns).reshape((TOKENS, TOP))
    act_b = gaussian(splits[3], (TOKENS, DW), 1.0, 6.0, ((0, 256),))
    grad_b = gaussian(splits[4], (TOKENS, TOP, FW), 0.02, 0.125, ((0, 256),))
    route_b_keys = jax.random.split(jax.random.fold_in(splits[5], 1), TOKENS // TOK_DEV)
    route_b_turns = jax.random.permutation(jax.random.fold_in(splits[5], 3), TOKENS // TOK_DEV)
    route_b = jax.vmap(lambda own, number: routed_block(jax.random.fold_in(splits[5], 2), own, number, TOK_DEV, EXP_B, TOP, 2 * MOST, 2))(route_b_keys, route_b_turns).reshape((TOKENS, TOP))
    return {"act_a": act_a, "grad_a": grad_a, "route_a": route_a, "act_b": act_b, "grad_b": grad_b, "route_b": route_b}


def slot_table(route, experts, stride, slot_count):
    flat_ids = route.reshape(DEVICES, TOK_DEV * TOP)
    onehot = (flat_ids[:, :, None] == jnp.arange(experts, dtype=jnp.int32)[None, None, :]).astype(jnp.int32)
    before = jnp.cumsum(onehot, axis=1) - onehot
    position = jnp.sum(before * onehot, axis=2).astype(jnp.int32)
    slot_index = (flat_ids * stride + position).astype(jnp.int32)
    pair_ids = jnp.broadcast_to(jnp.arange(TOK_DEV * TOP, dtype=jnp.int32)[None, :], flat_ids.shape)
    device_ids = jnp.broadcast_to(jnp.arange(DEVICES, dtype=jnp.int32)[:, None], flat_ids.shape)
    return jnp.full((DEVICES, slot_count), -1, jnp.int32).at[device_ids, slot_index].set(pair_ids)


def gather_rows(acts, grads, sources):
    filled = (sources >= 0).reshape(-1)[:, None]
    clamped = jnp.maximum(sources, 0)
    device_base = jnp.arange(DEVICES, dtype=jnp.int32)[:, None]
    token_ids = (device_base * TOK_DEV + clamped // TOP).reshape(-1).astype(jnp.int32)
    pair_index = (device_base * (TOK_DEV * TOP) + clamped).reshape(-1).astype(jnp.int32)
    rows_act = jnp.where(filled, acts[token_ids].astype(jnp.float32), jnp.float32(0.0))
    flat_grads = grads.reshape(TOKENS * TOP, FW)
    rows_grad = jnp.where(filled, flat_grads[pair_index].astype(jnp.float32), jnp.float32(0.0))
    return rows_act, rows_grad


def reference(act_a, grad_a, route_a, act_b, grad_b, route_b):
    table_a = slot_table(route_a, EXP_A, MOST, EXP_A * MOST)

    def expert_a(expert):
        sources = lax.dynamic_slice_in_dim(table_a, expert * MOST, MOST, 1)
        rows_act, rows_grad = gather_rows(act_a, grad_a, sources)
        summed = jnp.dot(rows_act.T, rows_grad, preferred_element_type=jnp.float32, precision=lax.Precision.HIGHEST)
        return summed.astype(jnp.bfloat16)

    wgrad_a = lax.map(expert_a, jnp.arange(EXP_A, dtype=jnp.int32))

    table_b = slot_table(route_b, EXP_B, 2 * MOST, EXP_B * 2 * MOST)

    def expert_b(expert):
        halves = []
        for half_index in range(2):
            sources = lax.dynamic_slice_in_dim(table_b, expert * (2 * MOST) + half_index * MOST, MOST, 1)
            rows_act, rows_grad = gather_rows(act_b, grad_b, sources)
            rows_act = rows_act.reshape(N_REP, N_EXP * MOST, DW)
            rows_grad = rows_grad.reshape(N_REP, N_EXP * MOST, FW)
            partial_value = jnp.einsum("rnd,rnf->rdf", rows_act, rows_grad, precision=lax.Precision.HIGHEST)
            halves.append(partial_value.astype(jnp.bfloat16))
        paired = (halves[0].astype(jnp.float32) + halves[1].astype(jnp.float32)).astype(jnp.bfloat16)
        paired = paired.reshape(N_REP, 2, DW // 2, FW)
        return jnp.sum(paired.astype(jnp.float32), axis=0).astype(jnp.bfloat16)

    wgrad_b = lax.map(expert_b, jnp.arange(EXP_B, dtype=jnp.int32)).reshape(2 * EXP_B, DW // 2, FW)
    return wgrad_a, wgrad_b
```

```python
import jax
import jax.numpy as jnp
from jax import lax
from jax.sharding import Mesh, PartitionSpec as P

Z = ("zh", "zl")
PLANE = ("x", "y", "c")
ALL = Z + PLANE
BF = jnp.bfloat16


def contract(left, right, dims):
    return lax.dot_general(left, right, (dims, ((), ())), preferred_element_type=jnp.float32)


def positions(ids):
    order = jnp.arange(ids.shape[0], dtype=jnp.int32)
    same = (ids[:, None] == ids[None, :]) & (order[:, None] < order[None, :])
    return jnp.sum(same.astype(jnp.int32), axis=0)


def one_hot(slots, count):
    return (jnp.arange(count, dtype=jnp.int32)[:, None] == slots[None, :]).astype(BF)


def shards(act_a, grad_a, route_a, act_b, grad_b, route_b):
    tokens, top = route_a.shape
    pairs = tokens * top
    features = act_a.shape[1]
    hidden = grad_a.shape[2]
    planes = lax.axis_size(Z)
    spots = lax.axis_size(PLANE)
    chips = spots // 2
    most = 5
    quarter = features // 4
    half = features // 2
    block = features // 8
    my_zl = lax.axis_index("zl")

    ids_a = route_a.reshape(-1)
    pos_a = positions(ids_a)
    info = jnp.zeros((8, hidden), BF)
    info = info.at[0, :pairs].set(ids_a.astype(BF)).at[1, :pairs].set(pos_a.astype(BF))
    grads_a = jnp.concatenate([grad_a.reshape(pairs, hidden), info], axis=0)
    all_grads = lax.all_gather(grads_a, Z, axis=0, tiled=True)
    my_zh = lax.axis_index("zh")
    my_z = 2 * my_zh + my_zl
    sign = 1 - 2 * my_zl
    quarters = jnp.moveaxis(act_a.reshape(tokens, 4, quarter), 1, 0)

    def mine(which):
        return lax.dynamic_index_in_dim(quarters, lax.rem(which + 8, 4), 0, keepdims=False)

    def along(block_in, step):
        return lax.ppermute(block_in, Z, [(z, (z + step * (1 - 2 * (z % 2))) % planes) for z in range(planes)])

    own = mine(my_zh)
    near = [own]
    for to, step in ((my_zh + 2, -3), (my_zh + sign, 2), (my_zh - sign, -1)):
        near.append(along(mine(to), step))
    offsets = (0, -3, -2, -1, 1, 4, 3, 2)
    origin = lax.rem(jnp.stack([my_z + o * sign for o in offsets]) + planes, planes)

    room = 24
    ids_b = route_b.reshape(-1)
    pos_b = positions(ids_b)
    slots_b = (ids_b % chips) * room + (ids_b // chips) * (room // 2) + pos_b
    pick_b = one_hot(slots_b, chips * room)
    pick_tok = one_hot(slots_b[0::2], chips * room) + one_hot(slots_b[1::2], chips * room)
    rows_g = contract(pick_b, grad_b.reshape(pairs, hidden), ((1,), (0,))).astype(BF)
    rows_a = contract(pick_tok, act_b, ((1,), (0,))).astype(BF)
    rows_g = jnp.broadcast_to(rows_g.reshape(chips, 1, room, hidden), (chips, 2, room, hidden))
    rows_a = jnp.moveaxis(rows_a.reshape(chips, room, 2, half), 2, 1)
    send_b = jnp.concatenate([rows_a, rows_g], axis=-1).reshape(spots, room, half + hidden)
    recv_b = lax.all_to_all(send_b, PLANE, 0, 0, tiled=True).reshape(spots * room, half + hidden)
    recv_b, near = lax.optimization_barrier((recv_b, near))
    far = [along(n, 1) for n in near]
    recv_ba, recv_bg = recv_b[:, :half], recv_b[:, half:]
    which = (jnp.arange(spots * room, dtype=jnp.int32) % room) // (room // 2)
    parts = [
        contract(jnp.where((which == k)[:, None], recv_ba, jnp.zeros((), BF)), recv_bg, ((0,), (0,))).astype(BF)
        for k in range(2)
    ]
    parts = jnp.stack([p.reshape(4, block, hidden) for p in parts], axis=1).reshape(features, hidden)
    parts, far = lax.optimization_barrier((parts, far))
    acts_in = jnp.concatenate(near + far, axis=0)
    wgrad_b = lax.psum_scatter(parts, Z, scatter_dimension=0, tiled=True)[None]

    info_in = all_grads.reshape(planes, pairs + 8, hidden)[:, pairs : pairs + 2, :pairs]
    ids = info_in[:, 0].astype(jnp.int32)
    pos = info_in[:, 1].astype(jnp.int32)
    src = jnp.arange(planes, dtype=jnp.int32)[:, None]
    slots = (ids % spots) * (planes * most) + src * most + pos
    slots = jnp.where(ids // spots == my_zl, slots, -1)
    total = spots * planes * most
    slots_g = jnp.concatenate([slots, jnp.full((planes, 8), -1, jnp.int32)], axis=1).reshape(-1)
    rows_g = contract(one_hot(slots_g, total), all_grads, ((1,), (0,))).astype(BF)
    slots_t = slots[origin]
    pick_tok = one_hot(slots_t[:, 0::2].reshape(-1), total) + one_hot(slots_t[:, 1::2].reshape(-1), total)
    rows_a = contract(pick_tok, acts_in, ((1,), (0,))).astype(BF)
    recv_g = lax.all_to_all(rows_g, PLANE, 0, 0, tiled=True)
    recv_a = lax.all_to_all(rows_a, PLANE, 0, 0, tiled=True)
    wgrad_a = contract(recv_a, recv_g, ((0,), (0,))).astype(BF)[None]
    return wgrad_a, wgrad_b


def solution(mesh):
    fine = Mesh(mesh.devices.reshape(4, 2, 4, 4, 2), ALL)
    return jax.shard_map(
        shards,
        mesh=fine,
        in_specs=tuple(P(ALL, *([None] * n)) for n in (1, 2, 1, 1, 2, 1)),
        out_specs=(P(("zl",) + PLANE, "zh", None),) * 2,
        check_vma=False,
    )
```

```python
import functools

import jax
import jax.numpy as jnp
from jax import lax
from jax.experimental import pallas as pl
from jax.sharding import Mesh, PartitionSpec as P

Z = ("zh", "zl")
PLANE = ("x", "y", "c")
ALL = Z + PLANE
BF = jnp.bfloat16
ROOM = 24


def contract(left, right, dims):
    return lax.dot_general(left, right, (dims, ((), ())), preferred_element_type=jnp.float32)


def positions(ids):
    order = jnp.arange(ids.shape[0], dtype=jnp.int32)
    same = (ids[:, None] == ids[None, :]) & (order[:, None] < order[None, :])
    return jnp.sum(same.astype(jnp.int32), axis=0)


def one_hot(slots, count):
    return (jnp.arange(count, dtype=jnp.int32)[:, None] == slots[None, :]).astype(BF)


def fill_kernel(half, s_ref, t_ref, act_ref, grad_ref, out_ref):
    chips = out_ref.shape[0]
    rows = chips * ROOM
    pairs = s_ref.shape[1]
    tokens = t_ref.shape[1]
    pick = (lax.broadcasted_iota(jnp.int32, (rows, pairs), 0) == s_ref[...]).astype(BF)
    spot = lax.broadcasted_iota(jnp.int32, (rows, tokens), 0)
    pick_tok = ((spot == t_ref[0:1, :]) | (spot == t_ref[1:2, :])).astype(BF)
    acts = contract(pick_tok, act_ref[...], ((1,), (0,))).astype(BF)
    grads = contract(pick, grad_ref[...], ((1,), (0,))).astype(BF)
    for p in range(chips):
        out_ref[p, 0, :, :half] = acts[p * ROOM : (p + 1) * ROOM]
        out_ref[p, 0, :, half:] = grads[p * ROOM : (p + 1) * ROOM]


def fill(slots, act, grad, chips):
    tokens, features = act.shape
    pairs, hidden = grad.shape
    half = features // 2
    return pl.pallas_call(
        functools.partial(fill_kernel, half),
        grid=(2,),
        in_specs=[
            pl.BlockSpec((1, pairs), lambda c: (0, 0)),
            pl.BlockSpec((2, tokens), lambda c: (0, 0)),
            pl.BlockSpec((tokens, half), lambda c: (0, c)),
            pl.BlockSpec((pairs, hidden), lambda c: (0, 0)),
        ],
        out_specs=pl.BlockSpec((chips, 1, ROOM, half + hidden), lambda c: (0, c, 0, 0)),
        out_shape=jax.ShapeDtypeStruct((chips, 2, ROOM, half + hidden), BF),
        cost_estimate=pl.CostEstimate(flops=2_000_000_000, bytes_accessed=6_000_000, transcendentals=0),
        name="fill_b",
    )(slots.reshape(1, pairs), slots.reshape(tokens, 2).T, act, grad)


def products_kernel(half, block, in_ref, out_ref):
    count = in_ref.shape[0] * 8
    hidden = in_ref.shape[2] - half

    def rows(tile, start, size):
        return in_ref[:, pl.ds(tile * 8, 8), start : start + size].reshape(count, size)

    shared = (lax.broadcasted_iota(jnp.int32, (count, 1), 0) % 8) // 4
    for pair in range(2):
        for k in range(2):

            @pl.when((pl.program_id(0) == pair) & (pl.program_id(1) == k))
            def _():
                start = pair * 2 * block
                last = jnp.where(shared == k, rows(2, half, hidden), jnp.zeros((), BF))
                total = contract(rows(k, start, 2 * block), rows(k, half, hidden), ((0,), (0,)))
                total = total + contract(rows(2, start, 2 * block), last, ((0,), (0,)))
                out_ref[...] = total.astype(BF).reshape(out_ref.shape)


def products(recv, half):
    hidden = recv.shape[2] - half
    block = half // 4
    return pl.pallas_call(
        functools.partial(products_kernel, half, block),
        grid=(2, 2),
        in_specs=[pl.BlockSpec(recv.shape, lambda r, k: (0, 0, 0))],
        out_specs=pl.BlockSpec((2, 1, block, hidden), lambda r, k: (r, k, 0, 0)),
        out_shape=jax.ShapeDtypeStruct((4, 2, block, hidden), BF),
        cost_estimate=pl.CostEstimate(flops=4_000_000_000, bytes_accessed=12_000_000, transcendentals=0),
        name="products_b",
    )(recv)


def shards(act_a, grad_a, route_a, act_b, grad_b, route_b):
    tokens, top = route_a.shape
    pairs = tokens * top
    features = act_a.shape[1]
    hidden = grad_a.shape[2]
    planes = lax.axis_size(Z)
    spots = lax.axis_size(PLANE)
    chips = spots // 2
    most = 5
    quarter = features // 4
    half = features // 2
    my_zh = lax.axis_index("zh")
    my_zl = lax.axis_index("zl")
    my_z = 2 * my_zh + my_zl
    sign = 1 - 2 * my_zl

    all_grads = lax.all_gather(grad_a.reshape(pairs, hidden), Z, axis=0, tiled=True)
    quarters = jnp.moveaxis(act_a.reshape(tokens, 4, quarter), 1, 0)

    def mine(which):
        return lax.dynamic_index_in_dim(quarters, lax.rem(which + 8, 4), 0, keepdims=False)

    def along(block_in, step):
        return lax.ppermute(block_in, Z, [(z, (z + step * (1 - 2 * (z % 2))) % planes) for z in range(planes)])

    near = [mine(my_zh)]
    for to, step in ((my_zh + 2, -3), (my_zh + sign, 2), (my_zh - sign, -1)):
        near.append(along(mine(to), step))
    offsets = (0, -3, -2, -1, 1, 4, 3, 2)
    origin = lax.rem(jnp.stack([my_z + o * sign for o in offsets]) + planes, planes)

    ids_b = route_b.reshape(-1)
    pos_b = positions(ids_b)
    lower = ids_b // chips
    slots_b = (ids_b % chips) * ROOM + jnp.where(pos_b < 8, lower * 8 + pos_b, 16 + lower * 4 + pos_b - 8)
    send_b = fill(slots_b, act_b, grad_b.reshape(pairs, hidden), chips)
    recv_b = lax.all_to_all(send_b.reshape(spots, ROOM, half + hidden), PLANE, 0, 0, tiled=True)

    ids_a = route_a.reshape(-1)
    slots_a = (ids_a % spots) * (planes * most) + my_z * most + positions(ids_a)
    slots_a = slots_a + (ids_a // spots) * 4096
    slots_a, _ = lax.optimization_barrier((slots_a, send_b))
    slots = lax.all_gather(slots_a, Z, axis=0)
    slots = jnp.where(slots // 4096 == my_zl, slots % 4096, -1)

    far = [along(b, 1) for b in near]
    parts = products(recv_b, half).reshape(features, hidden)
    parts, far = lax.optimization_barrier((parts, far))
    wgrad_b = lax.psum_scatter(parts, Z, scatter_dimension=0, tiled=True)[None]

    total = spots * planes * most
    slots_t = slots[origin]
    pick_tok = one_hot(slots_t[:, 0::2].reshape(-1), total) + one_hot(slots_t[:, 1::2].reshape(-1), total)
    rows_a = contract(pick_tok, jnp.concatenate(near + far, axis=0), ((1,), (0,))).astype(BF)
    recv_a = lax.all_to_all(rows_a, PLANE, 0, 0, tiled=True)
    rows_g = contract(one_hot(slots.reshape(-1), total), all_grads, ((1,), (0,))).astype(BF)
    recv_g = lax.all_to_all(rows_g, PLANE, 0, 0, tiled=True)
    wgrad_a = contract(recv_a, recv_g, ((0,), (0,))).astype(BF)[None]
    return wgrad_a, wgrad_b


def solution(mesh):
    fine = Mesh(mesh.devices.reshape(4, 2, 4, 4, 2), ALL)
    return jax.shard_map(
        shards,
        mesh=fine,
        in_specs=tuple(P(ALL, *([None] * n)) for n in (1, 2, 1, 1, 2, 1)),
        out_specs=(P(("zl",) + PLANE, "zh", None),) * 2,
        check_vma=False,
    )
```

```python
import functools

import jax
import jax.numpy as jnp
from jax import lax
from jax.experimental import pallas as pl
from jax.sharding import Mesh, PartitionSpec as P

Z = ("zh", "zl")
PLANE = ("x", "y", "c")
ALL = Z + PLANE
BF = jnp.bfloat16
TILE = 8


def contract(left, right, dims):
    return lax.dot_general(left, right, (dims, ((), ())), preferred_element_type=jnp.float32)


def positions(ids):
    order = jnp.arange(ids.shape[0], dtype=jnp.int32)
    same = (ids[:, None] == ids[None, :]) & (order[:, None] < order[None, :])
    return jnp.sum(same.astype(jnp.int32), axis=0)


def one_hot(slots, count):
    return (jnp.arange(count, dtype=jnp.int32)[:, None] == slots[None, :]).astype(BF)


def fill_kernel(half, s_ref, t_ref, act_ref, grad_ref, out_ref):
    chips = out_ref.shape[0]
    rows = chips * TILE
    pairs = s_ref.shape[1]
    tokens = t_ref.shape[1]
    width = half + grad_ref.shape[1]
    quarter = half // 2
    lower = lax.broadcasted_iota(jnp.int32, (rows, 1), 0) % TILE < TILE // 2
    for tile in range(3):

        def spots(count):
            row = lax.broadcasted_iota(jnp.int32, (rows, count), 0)
            if tile == 2:
                row = row - row % TILE + row % (TILE // 2)
            return row + tile * rows

        pick = (spots(pairs) == s_ref[...]).astype(BF)
        spot = spots(tokens)
        pick_tok = ((spot == t_ref[0:1, :]) | (spot == t_ref[1:2, :])).astype(BF)
        acts = contract(pick_tok, act_ref[...], ((1,), (0,))).astype(BF)
        grads = contract(pick, grad_ref[...], ((1,), (0,))).astype(BF)
        if tile == 2:
            acts = jnp.where(lower, acts[:, :quarter], acts[:, quarter:])
        start = tile * width
        middle = start + acts.shape[1]
        for p in range(chips):
            out_ref[p, 0, :, start:middle] = acts[p * TILE : (p + 1) * TILE]
            out_ref[p, 0, :, middle : middle + grads.shape[1]] = grads[p * TILE : (p + 1) * TILE]


def fill(slots, act, grad, chips):
    tokens, features = act.shape
    pairs, hidden = grad.shape
    half = features // 2
    width = 2 * (half + hidden) + half // 2 + hidden
    return pl.pallas_call(
        functools.partial(fill_kernel, half),
        grid=(2,),
        in_specs=[
            pl.BlockSpec((1, pairs), lambda c: (0, 0)),
            pl.BlockSpec((2, tokens), lambda c: (0, 0)),
            pl.BlockSpec((tokens, half), lambda c: (0, c)),
            pl.BlockSpec((pairs, hidden), lambda c: (0, 0)),
        ],
        out_specs=pl.BlockSpec((chips, 1, TILE, width), lambda c: (0, c, 0, 0)),
        out_shape=jax.ShapeDtypeStruct((chips, 2, TILE, width), BF),
        cost_estimate=pl.CostEstimate(flops=2_000_000_000, bytes_accessed=6_000_000, transcendentals=0),
        name="fill_b",
    )(slots.reshape(1, pairs), slots.reshape(tokens, 2).T, act, grad)


def products_kernel(half, hidden, in_ref, out_ref):
    count = in_ref.shape[0] * TILE
    quarter = half // 2
    width = half + hidden

    def rows(start, size):
        return in_ref[:, :, start : start + size].reshape(count, size)

    row = lax.broadcasted_iota(jnp.int32, (count, 1), 0) % TILE
    for pair in range(2):
        for k in range(2):

            @pl.when((pl.program_id(0) == pair) & (pl.program_id(1) == k))
            def _():
                owner = row // 2 == pair * 2 + k
                last = jnp.where(owner, rows(2 * width + quarter, hidden), jnp.zeros((), BF))
                total = contract(rows(k * width + pair * quarter, quarter), rows(k * width + half, hidden), ((0,), (0,)))
                total = total + contract(rows(2 * width, quarter), last, ((0,), (0,)))
                out_ref[...] = total.astype(BF).reshape(out_ref.shape)


def products(recv, half, hidden):
    block = half // 4
    return pl.pallas_call(
        functools.partial(products_kernel, half, hidden),
        grid=(2, 2),
        in_specs=[pl.BlockSpec(recv.shape, lambda r, k: (0, 0, 0))],
        out_specs=pl.BlockSpec((2, 1, block, hidden), lambda r, k: (r, k, 0, 0)),
        out_shape=jax.ShapeDtypeStruct((4, 2, block, hidden), BF),
        cost_estimate=pl.CostEstimate(flops=4_000_000_000, bytes_accessed=12_000_000, transcendentals=0),
        name="products_b",
    )(recv)


def shards(act_a, grad_a, route_a, act_b, grad_b, route_b):
    tokens, top = route_a.shape
    pairs = tokens * top
    features = act_a.shape[1]
    hidden = grad_a.shape[2]
    planes = lax.axis_size(Z)
    spots = lax.axis_size(PLANE)
    chips = spots // 2
    most = 5
    quarter = features // 4
    half = features // 2
    my_zh = lax.axis_index("zh")
    my_zl = lax.axis_index("zl")
    my_z = 2 * my_zh + my_zl
    sign = 1 - 2 * my_zl

    all_grads = lax.all_gather(grad_a.reshape(pairs, hidden), Z, axis=0, tiled=True)
    quarters = jnp.moveaxis(act_a.reshape(tokens, 4, quarter), 1, 0)

    def mine(which):
        return lax.dynamic_index_in_dim(quarters, lax.rem(which + 8, 4), 0, keepdims=False)

    def along(block_in, step):
        return lax.ppermute(block_in, Z, [(z, (z + step * (1 - 2 * (z % 2))) % planes) for z in range(planes)])

    near = [mine(my_zh)]
    for to, step in ((my_zh + 2, -3), (my_zh + sign, 2), (my_zh - sign, -1)):
        near.append(along(mine(to), step))
    offsets = (0, -3, -2, -1, 1, 4, 3, 2)
    origin = lax.rem(jnp.stack([my_z + o * sign for o in offsets]) + planes, planes)

    ids_b = route_b.reshape(-1)
    pos_b = positions(ids_b)
    lower = ids_b // chips
    row_b = jnp.where(pos_b < TILE, lower * (chips * TILE) + pos_b, 2 * chips * TILE + lower * 2 + pos_b - TILE)
    slots_b = (ids_b % chips) * TILE + row_b
    send_b = fill(slots_b, act_b, grad_b.reshape(pairs, hidden), chips)
    recv_b = lax.all_to_all(send_b.reshape(spots, TILE, send_b.shape[-1]), PLANE, 0, 0, tiled=True)

    ids_a = route_a.reshape(-1)
    slots_a = (ids_a % spots) * (planes * most) + my_z * most + positions(ids_a)
    slots_a = slots_a + (ids_a // spots) * 4096
    slots_a, _ = lax.optimization_barrier((slots_a, send_b))
    slots = lax.all_gather(slots_a, Z, axis=0)
    slots = jnp.where(slots // 4096 == my_zl, slots % 4096, -1)

    far = [along(b, 1) for b in near]
    parts = products(recv_b, half, hidden).reshape(features, hidden)
    parts, far = lax.optimization_barrier((parts, far))
    wgrad_b = lax.psum_scatter(parts, Z, scatter_dimension=0, tiled=True)[None]

    total = spots * planes * most
    slots_t = slots[origin]
    pick_tok = one_hot(slots_t[:, 0::2].reshape(-1), total) + one_hot(slots_t[:, 1::2].reshape(-1), total)
    rows_a = contract(pick_tok, jnp.concatenate(near + far, axis=0), ((1,), (0,))).astype(BF)
    recv_a = lax.all_to_all(rows_a, PLANE, 0, 0, tiled=True)
    rows_g = contract(one_hot(slots.reshape(-1), total), all_grads, ((1,), (0,))).astype(BF)
    recv_g = lax.all_to_all(rows_g, PLANE, 0, 0, tiled=True)
    wgrad_a = contract(recv_a, recv_g, ((0,), (0,))).astype(BF)[None]
    return wgrad_a, wgrad_b


def solution(mesh):
    fine = Mesh(mesh.devices.reshape(4, 2, 4, 4, 2), ALL)
    return jax.shard_map(
        shards,
        mesh=fine,
        in_specs=tuple(P(ALL, *([None] * n)) for n in (1, 2, 1, 1, 2, 1)),
        out_specs=(P(("zl",) + PLANE, "zh", None),) * 2,
        check_vma=False,
    )
```

```python
import functools

import jax
import jax.numpy as jnp
from jax import lax
from jax.experimental import pallas as pl
from jax.sharding import Mesh, PartitionSpec as P

Z = ("zh", "zl")
PLANE = ("x", "y", "c")
ALL = Z + PLANE
BF = jnp.bfloat16
TILE = 8


def contract(left, right, dims):
    return lax.dot_general(left, right, (dims, ((), ())), preferred_element_type=jnp.float32)


def positions(ids):
    order = jnp.arange(ids.shape[0], dtype=jnp.int32)
    same = (ids[:, None] == ids[None, :]) & (order[:, None] < order[None, :])
    return jnp.sum(same.astype(jnp.int32), axis=0)


def one_hot(slots, count):
    return (jnp.arange(count, dtype=jnp.int32)[:, None] == slots[None, :]).astype(BF)


def fill_kernel(half, s_ref, t_ref, act_ref, grad_ref, out_ref):
    chips = out_ref.shape[0]
    rows = chips * TILE
    pairs = s_ref.shape[1]
    tokens = t_ref.shape[1]
    width = half + grad_ref.shape[1]
    quarter = half // 2
    lower = lax.broadcasted_iota(jnp.int32, (rows, 1), 0) % TILE < TILE // 2
    for tile in range(3):

        def spots(count):
            row = lax.broadcasted_iota(jnp.int32, (rows, count), 0)
            if tile == 2:
                row = row - row % TILE + row % (TILE // 2)
            return row + tile * rows

        pick = (spots(pairs) == s_ref[...]).astype(BF)
        spot = spots(tokens)
        pick_tok = ((spot == t_ref[0:1, :]) | (spot == t_ref[1:2, :])).astype(BF)
        acts = contract(pick_tok, act_ref[...], ((1,), (0,))).astype(BF)
        grads = contract(pick, grad_ref[...], ((1,), (0,))).astype(BF)
        if tile == 2:
            acts = jnp.where(lower, acts[:, :quarter], acts[:, quarter:])
        start = tile * width
        middle = start + acts.shape[1]
        for p in range(chips):
            out_ref[p, 0, :, start:middle] = acts[p * TILE : (p + 1) * TILE]
            out_ref[p, 0, :, middle : middle + grads.shape[1]] = grads[p * TILE : (p + 1) * TILE]


def fill(slots, act, grad, chips):
    tokens, features = act.shape
    pairs, hidden = grad.shape
    half = features // 2
    width = 2 * (half + hidden) + half // 2 + hidden
    return pl.pallas_call(
        functools.partial(fill_kernel, half),
        grid=(2,),
        in_specs=[
            pl.BlockSpec((1, pairs), lambda c: (0, 0)),
            pl.BlockSpec((2, tokens), lambda c: (0, 0)),
            pl.BlockSpec((tokens, half), lambda c: (0, c)),
            pl.BlockSpec((pairs, hidden), lambda c: (0, 0)),
        ],
        out_specs=pl.BlockSpec((chips, 1, TILE, width), lambda c: (0, c, 0, 0)),
        out_shape=jax.ShapeDtypeStruct((chips, 2, TILE, width), BF),
        cost_estimate=pl.CostEstimate(flops=2_000_000_000, bytes_accessed=6_000_000, transcendentals=0),
        name="fill_b",
    )(slots.reshape(1, pairs), slots.reshape(tokens, 2).T, act, grad)


def products_kernel(half, hidden, in_ref, out_ref):
    count = in_ref.shape[0] * TILE
    quarter = half // 2
    width = half + hidden

    def rows(start, size):
        return in_ref[:, :, start : start + size].reshape(count, size)

    row = lax.broadcasted_iota(jnp.int32, (count, 1), 0) % TILE
    for pair in range(2):
        for k in range(2):

            @pl.when((pl.program_id(0) == pair) & (pl.program_id(1) == k))
            def _():
                owner = row // 2 == pair * 2 + k
                last = jnp.where(owner, rows(2 * width + quarter, hidden), jnp.zeros((), BF))
                total = contract(rows(k * width + pair * quarter, quarter), rows(k * width + half, hidden), ((0,), (0,)))
                total = total + contract(rows(2 * width, quarter), last, ((0,), (0,)))
                out_ref[...] = total.astype(BF).reshape(out_ref.shape)


def products(recv, half, hidden):
    block = half // 4
    return pl.pallas_call(
        functools.partial(products_kernel, half, hidden),
        grid=(2, 2),
        in_specs=[pl.BlockSpec(recv.shape, lambda r, k: (0, 0, 0))],
        out_specs=pl.BlockSpec((2, 1, block, hidden), lambda r, k: (r, k, 0, 0)),
        out_shape=jax.ShapeDtypeStruct((4, 2, block, hidden), BF),
        cost_estimate=pl.CostEstimate(flops=4_000_000_000, bytes_accessed=12_000_000, transcendentals=0),
        name="products_b",
    )(recv)


def ordered(block_in, target):
    planes = lax.axis_size(Z)
    return lax.ppermute(block_in, Z, [(z, target(z) % planes) for z in range(planes)])


def shards(act_a, grad_a, route_a, act_b, grad_b, route_b):
    tokens, top = route_a.shape
    pairs = tokens * top
    features = act_a.shape[1]
    hidden = grad_a.shape[2]
    planes = lax.axis_size(Z)
    spots = lax.axis_size(PLANE)
    chips = spots // 2
    most = 5
    quarter = features // 4
    half = features // 2
    my_zh = lax.axis_index("zh")
    my_zl = lax.axis_index("zl")
    my_z = 2 * my_zh + my_zl
    sign = 1 - 2 * my_zl

    ids_a = route_a.reshape(-1)
    info = jnp.stack([ids_a, positions(ids_a)]).astype(BF)
    info = jnp.pad(info, ((0, 6), (0, hidden - pairs)))
    grads = jnp.concatenate([grad_a.reshape(pairs, hidden), info], axis=0)
    up, down = [grads], [grads]
    for _ in range(1, 4):
        up.append(ordered(up[-1], lambda z: z + 1))
        down.append(ordered(down[-1], lambda z: z - 1))
    cut = pairs // 2
    across = jnp.concatenate(
        [ordered(up[3][:cut], lambda z: z + 1), ordered(down[3][cut:], lambda z: z - 1)],
        axis=0,
    )
    ring = (0, -1, -2, -3, 4, 3, 2, 1)
    all_grads = jnp.concatenate(up + [across] + down[:0:-1], axis=0)

    quarters = jnp.moveaxis(act_a.reshape(tokens, 4, quarter), 1, 0)

    def mine(which):
        return lax.dynamic_index_in_dim(quarters, lax.rem(which + 8, 4), 0, keepdims=False)

    def along(block_in, step):
        return ordered(block_in, lambda z: z + step * (1 - 2 * (z % 2)))

    near = [mine(my_zh)]
    for to, step in ((my_zh + 2, -3), (my_zh + sign, 2), (my_zh - sign, -1)):
        near.append(along(mine(to), step))
    offsets = (0, -3, -2, -1, 1, 4, 3, 2)
    far = [along(b, 1) for b in near]

    ids_b = route_b.reshape(-1)
    pos_b = positions(ids_b)
    lower = ids_b // chips
    row_b = jnp.where(pos_b < TILE, lower * (chips * TILE) + pos_b, 2 * chips * TILE + lower * 2 + pos_b - TILE)
    slots_b = (ids_b % chips) * TILE + row_b
    send_b = fill(slots_b, act_b, grad_b.reshape(pairs, hidden), chips)
    recv_b = lax.all_to_all(send_b.reshape(spots, TILE, send_b.shape[-1]), PLANE, 0, 0, tiled=True)

    parts = products(recv_b, half, hidden).reshape(features, hidden)
    wgrad_b = lax.psum_scatter(parts, Z, scatter_dimension=0, tiled=True)[None]

    total = spots * planes * most
    told = all_grads.reshape(planes, pairs + 8, hidden)[:, pairs : pairs + 2, :pairs].astype(jnp.int32)
    origin = lax.rem(jnp.stack([my_z + o for o in ring]) + planes, planes)
    slots = (told[:, 0] % spots) * (planes * most) + origin[:, None] * most + told[:, 1]
    slots = jnp.where(told[:, 0] // spots == my_zl, slots, -1)
    even = slots[jnp.array([ring.index(o) for o in offsets])]
    odd = slots[jnp.array([ring.index(-o if -o in ring else 4) for o in offsets])]
    slots_t = jnp.where(my_zl == 0, even, odd)
    pick_tok = one_hot(slots_t[:, 0::2].reshape(-1), total) + one_hot(slots_t[:, 1::2].reshape(-1), total)
    rows_a = contract(pick_tok, jnp.concatenate(near + far, axis=0), ((1,), (0,))).astype(BF)
    slots_g = jnp.pad(slots, ((0, 0), (0, 8)), constant_values=-1)
    rows_g = contract(one_hot(slots_g.reshape(-1), total), all_grads, ((1,), (0,))).astype(BF)
    recv_a = lax.all_to_all(rows_a, PLANE, 0, 0, tiled=True)
    recv_g = lax.all_to_all(rows_g, PLANE, 0, 0, tiled=True)
    wgrad_a = contract(recv_a, recv_g, ((0,), (0,))).astype(BF)[None]
    return wgrad_a, wgrad_b


def solution(mesh):
    fine = Mesh(mesh.devices.reshape(4, 2, 4, 4, 2), ALL)
    return jax.shard_map(
        shards,
        mesh=fine,
        in_specs=tuple(P(ALL, *([None] * n)) for n in (1, 2, 1, 1, 2, 1)),
        out_specs=(P(("zl",) + PLANE, "zh", None),) * 2,
        check_vma=False,
    )
```

```python
import functools

import jax
import jax.numpy as jnp
from jax import lax
from jax.experimental import pallas as pl
from jax.experimental.pallas import tpu as pltpu
from jax.sharding import Mesh, PartitionSpec as P

Z = ("zh", "zl")
PLANE = ("x", "y", "c")
ALL = Z + PLANE
BF = jnp.bfloat16
TILE = 8


def contract(left, right, dims):
    return lax.dot_general(left, right, (dims, ((), ())), preferred_element_type=jnp.float32)


def positions(ids):
    order = jnp.arange(ids.shape[0], dtype=jnp.int32)
    same = (ids[:, None] == ids[None, :]) & (order[:, None] < order[None, :])
    return jnp.sum(same.astype(jnp.int32), axis=0)


def fill_kernel(half, s_ref, t_ref, act_ref, grad_ref, out_ref):
    chips = out_ref.shape[0]
    rows = chips * TILE
    pairs = s_ref.shape[1]
    tokens = t_ref.shape[1]
    width = half + grad_ref.shape[1]
    quarter = half // 2
    lower = lax.broadcasted_iota(jnp.int32, (rows, 1), 0) % TILE < TILE // 2
    for tile in range(3):

        def spots(count):
            row = lax.broadcasted_iota(jnp.int32, (rows, count), 0)
            if tile == 2:
                row = row - row % TILE + row % (TILE // 2)
            return row + tile * rows

        pick = (spots(pairs) == s_ref[...]).astype(BF)
        spot = spots(tokens)
        pick_tok = ((spot == t_ref[0:1, :]) | (spot == t_ref[1:2, :])).astype(BF)
        acts = contract(pick_tok, act_ref[...], ((1,), (0,))).astype(BF)
        grads = contract(pick, grad_ref[...], ((1,), (0,))).astype(BF)
        if tile == 2:
            acts = jnp.where(lower, acts[:, :quarter], acts[:, quarter:])
        start = tile * width
        middle = start + acts.shape[1]
        for p in range(chips):
            out_ref[p, 0, :, start:middle] = acts[p * TILE : (p + 1) * TILE]
            out_ref[p, 0, :, middle : middle + grads.shape[1]] = grads[p * TILE : (p + 1) * TILE]


def fill(slots, act, grad, chips):
    tokens, features = act.shape
    pairs, hidden = grad.shape
    half = features // 2
    width = 2 * (half + hidden) + half // 2 + hidden
    return pl.pallas_call(
        functools.partial(fill_kernel, half),
        grid=(2,),
        in_specs=[
            pl.BlockSpec((1, pairs), lambda c: (0, 0)),
            pl.BlockSpec((2, tokens), lambda c: (0, 0)),
            pl.BlockSpec((tokens, half), lambda c: (0, c)),
            pl.BlockSpec((pairs, hidden), lambda c: (0, 0)),
        ],
        out_specs=pl.BlockSpec((chips, 1, TILE, width), lambda c: (0, c, 0, 0)),
        out_shape=jax.ShapeDtypeStruct((chips, 2, TILE, width), BF),
        cost_estimate=pl.CostEstimate(flops=2_000_000_000, bytes_accessed=6_000_000, transcendentals=0),
        name="fill_b",
    )(slots.reshape(1, pairs), slots.reshape(tokens, 2).T, act, grad)


def products_kernel(half, hidden, in_ref, out_ref):
    count = in_ref.shape[0] * TILE
    quarter = half // 2
    width = half + hidden

    def rows(start, size):
        return in_ref[:, :, start : start + size].reshape(count, size)

    row = lax.broadcasted_iota(jnp.int32, (count, 1), 0) % TILE
    for pair in range(2):
        for k in range(2):

            @pl.when((pl.program_id(0) == pair) & (pl.program_id(1) == k))
            def _():
                owner = row // 2 == pair * 2 + k
                last = jnp.where(owner, rows(2 * width + quarter, hidden), jnp.zeros((), BF))
                total = contract(rows(k * width + pair * quarter, quarter), rows(k * width + half, hidden), ((0,), (0,)))
                total = total + contract(rows(2 * width, quarter), last, ((0,), (0,)))
                out_ref[...] = total.astype(BF).reshape(out_ref.shape)


def products(recv, half, hidden):
    block = half // 4
    return pl.pallas_call(
        functools.partial(products_kernel, half, hidden),
        grid=(2, 2),
        in_specs=[pl.BlockSpec(recv.shape, lambda r, k: (0, 0, 0))],
        out_specs=pl.BlockSpec((2, 1, block, hidden), lambda r, k: (r, k, 0, 0)),
        out_shape=jax.ShapeDtypeStruct((4, 2, block, hidden), BF),
        cost_estimate=pl.CostEstimate(flops=4_000_000_000, bytes_accessed=12_000_000, transcendentals=0),
        name="products_b",
    )(recv)


def sort_acts_kernel(spots, most, meta_ref, *refs):
    blocks, rows_ref, slots_ref, held = refs[:8], refs[8], refs[9], refs[10]
    tokens = slots_ref.shape[1] // 2
    base = pl.program_id(0) * rows_ref.shape[0]
    row = lax.broadcasted_iota(jnp.int32, (rows_ref.shape[0], tokens), 0) + base
    picks = []
    for n, block in enumerate(blocks):
        told = block[tokens : tokens + 8, :tokens].astype(jnp.float32).astype(jnp.int32)
        pick = None
        for k in range(2):
            expert, pos = told[2 * k : 2 * k + 1], told[2 * k + 1 : 2 * k + 2]
            slot = (expert % spots) * (8 * most) + meta_ref[n] * most + pos
            slot = jnp.where(expert // spots == meta_ref[8], slot, -1)
            slots_ref[n : n + 1, k * tokens : (k + 1) * tokens] = slot
            hit = row == slot
            pick = hit if pick is None else pick | hit
        picks.append(pick.astype(BF))

    @pl.when(pl.program_id(0) == 0)
    def _():
        for n, block in enumerate(blocks):
            held[n * tokens : (n + 1) * tokens, :] = block[:tokens, :]

    rows_ref[...] = contract(jnp.concatenate(picks, axis=1), held[...], ((1,), (0,))).astype(BF)


def sort_acts(blocks, meta, tokens, spots, most):
    width = blocks[0].shape[1]
    total = spots * 8 * most
    return pl.pallas_call(
        functools.partial(sort_acts_kernel, spots, most),
        grid=(2,),
        in_specs=[pl.BlockSpec(memory_space=pltpu.SMEM)] + [pl.BlockSpec(b.shape, lambda i: (0, 0)) for b in blocks],
        out_specs=[pl.BlockSpec((total // 2, width), lambda i: (i, 0)), pl.BlockSpec((8, 2 * tokens), lambda i: (0, 0))],
        out_shape=[jax.ShapeDtypeStruct((total, width), BF), jax.ShapeDtypeStruct((8, 2 * tokens), jnp.int32)],
        scratch_shapes=[pltpu.VMEM((8 * tokens, width), BF)],
        cost_estimate=pl.CostEstimate(flops=2_400_000_000, bytes_accessed=5_000_000, transcendentals=0),
        name="sort_acts",
    )(meta, *blocks)


def sort_grads_kernel(at_ref, slots_ref, *refs):
    parts, rows_ref, held = refs[:-2], refs[-2], refs[-1]
    pairs = slots_ref.shape[1]
    base = pl.program_id(0) * rows_ref.shape[0]
    row = lax.broadcasted_iota(jnp.int32, (rows_ref.shape[0], pairs), 0) + base

    @pl.when(pl.program_id(0) == 0)
    def _():
        start = 0
        for part in parts:
            held[start : start + part.shape[0], :] = part[...]
            start += part.shape[0]

    picks = [(row == slots_ref[pl.ds(at_ref[n], 1), :]).astype(BF) for n in range(8)]
    rows_ref[...] = contract(jnp.concatenate(picks, axis=1), held[...], ((1,), (0,))).astype(BF)


def sort_grads(parts, slots, at, total):
    width = parts[0].shape[1]
    pairs = slots.shape[1]
    return pl.pallas_call(
        sort_grads_kernel,
        grid=(2,),
        in_specs=[pl.BlockSpec(memory_space=pltpu.SMEM), pl.BlockSpec(slots.shape, lambda i: (0, 0))]
        + [pl.BlockSpec(p.shape, lambda i: (0, 0)) for p in parts],
        out_specs=pl.BlockSpec((total // 2, width), lambda i: (i, 0)),
        out_shape=jax.ShapeDtypeStruct((total, width), BF),
        scratch_shapes=[pltpu.VMEM((8 * pairs, width), BF)],
        cost_estimate=pl.CostEstimate(flops=5_400_000_000, bytes_accessed=7_000_000, transcendentals=0),
        name="sort_grads",
    )(at, slots, *parts)


def ordered(block_in, target):
    planes = lax.axis_size(Z)
    return lax.ppermute(block_in, Z, [(z, target(z) % planes) for z in range(planes)])


def shards(act_a, grad_a, route_a, act_b, grad_b, route_b):
    tokens, top = route_a.shape
    pairs = tokens * top
    features = act_a.shape[1]
    hidden = grad_a.shape[2]
    planes = lax.axis_size(Z)
    spots = lax.axis_size(PLANE)
    chips = spots // 2
    most = 5
    quarter = features // 4
    half = features // 2
    my_zh = lax.axis_index("zh")
    my_zl = lax.axis_index("zl")
    my_z = 2 * my_zh + my_zl
    sign = 1 - 2 * my_zl

    grads = jnp.moveaxis(grad_a, 1, 0).reshape(pairs, hidden)
    up, down = [grads], [grads]
    for _ in range(1, 4):
        up.append(ordered(up[-1], lambda z: z + 1))
        down.append(ordered(down[-1], lambda z: z - 1))
    across = [ordered(up[3][:tokens], lambda z: z + 1), ordered(down[3][tokens:], lambda z: z - 1)]
    ring = (0, -1, -2, -3, 4, 3, 2, 1)

    ids_a = route_a.reshape(-1)
    info = jnp.stack([ids_a, positions(ids_a)]).reshape(2, tokens, top)
    info = jnp.moveaxis(info, 2, 0).reshape(2 * top, tokens).astype(BF)
    info = jnp.pad(info, ((0, 8 - 2 * top), (0, quarter - tokens)))
    quarters = jnp.moveaxis(act_a.reshape(tokens, 4, quarter), 1, 0)

    def mine(which):
        rows = lax.dynamic_index_in_dim(quarters, lax.rem(which + 8, 4), 0, keepdims=False)
        return jnp.concatenate([rows, info], axis=0)

    def along(block_in, step):
        return ordered(block_in, lambda z: z + step * (1 - 2 * (z % 2)))

    near = [mine(my_zh)]
    for to, step in ((my_zh + 2, -3), (my_zh + sign, 2), (my_zh - sign, -1)):
        near.append(along(mine(to), step))
    offsets = (0, -3, -2, -1, 1, 4, 3, 2)
    far = [along(b, 1) for b in near]

    ids_b = route_b.reshape(-1)
    pos_b = positions(ids_b)
    lower = ids_b // chips
    row_b = jnp.where(pos_b < TILE, lower * (chips * TILE) + pos_b, 2 * chips * TILE + lower * 2 + pos_b - TILE)
    slots_b = (ids_b % chips) * TILE + row_b
    send_b = fill(slots_b, act_b, grad_b.reshape(pairs, hidden), chips)
    recv_b = lax.all_to_all(send_b.reshape(spots, TILE, send_b.shape[-1]), PLANE, 0, 0, tiled=True)

    parts = products(recv_b, half, hidden).reshape(features, hidden)
    wgrad_b = lax.psum_scatter(parts, Z, scatter_dimension=0, tiled=True)[None]

    total = spots * planes * most
    origin = [lax.rem(my_z + o * sign + planes, planes) for o in offsets]
    rows_a, slots = sort_acts(near + far, jnp.stack(origin + [my_zl]), tokens, spots, most)
    even = [offsets.index(o) for o in ring]
    odd = [offsets.index(-o if -o in offsets else 4) for o in ring]
    at = jnp.stack([jnp.where(my_zl == 0, e, o).astype(jnp.int32) for e, o in zip(even, odd)])
    rows_g = sort_grads(up + across + down[:0:-1], slots, at, total)
    rows_a = rows_a.reshape(spots, planes * most, quarter)
    rows_g = rows_g.reshape(spots, planes * most, hidden)
    recv_a = lax.all_to_all(rows_a, PLANE, 0, 0, tiled=True).reshape(total, quarter)
    recv_g = lax.all_to_all(rows_g, PLANE, 0, 0, tiled=True).reshape(total, hidden)
    wgrad_a = contract(recv_a, recv_g, ((0,), (0,))).astype(BF)[None]
    return wgrad_a, wgrad_b


def solution(mesh):
    fine = Mesh(mesh.devices.reshape(4, 2, 4, 4, 2), ALL)
    return jax.shard_map(
        shards,
        mesh=fine,
        in_specs=tuple(P(ALL, *([None] * n)) for n in (1, 2, 1, 1, 2, 1)),
        out_specs=(P(("zl",) + PLANE, "zh", None),) * 2,
        check_vma=False,
    )
```

```python
import functools

import jax
import jax.numpy as jnp
from jax import lax
from jax.experimental import pallas as pl
from jax.experimental.pallas import tpu as pltpu
from jax.sharding import Mesh, PartitionSpec as P

Z = ("zh", "zl")
PLANE = ("x", "y", "c")
ALL = Z + PLANE
BF = jnp.bfloat16
TILE = 8


def contract(left, right, dims):
    return lax.dot_general(left, right, (dims, ((), ())), preferred_element_type=jnp.float32)


def positions(ids):
    order = jnp.arange(ids.shape[0], dtype=jnp.int32)
    same = (ids[:, None] == ids[None, :]) & (order[:, None] < order[None, :])
    return jnp.sum(same.astype(jnp.int32), axis=0)


def fill_kernel(half, ids_ref, act_ref, grad_ref, out_ref):
    chips = out_ref.shape[0]
    rows = chips * TILE
    tokens = ids_ref.shape[1]
    pairs = 2 * tokens
    width = half + grad_ref.shape[1]
    quarter = half // 2
    ids = jnp.concatenate([ids_ref[0:1, :], ids_ref[1:2, :]], axis=1)
    named = (lax.broadcasted_iota(jnp.int32, (2 * chips, pairs), 0) == ids).astype(jnp.float32)
    earlier = lax.broadcasted_iota(jnp.int32, (pairs, pairs), 0) < lax.broadcasted_iota(jnp.int32, (pairs, pairs), 1)
    before = contract(named.astype(BF), earlier.astype(BF), ((1,), (0,)))
    pos = jnp.sum(named * before, axis=0, keepdims=True).astype(jnp.int32)
    expert = ids // chips
    row = jnp.where(pos < TILE, expert * rows + pos, 2 * rows + expert * 2 + pos - TILE)
    slots = (ids % chips) * TILE + row
    lower = lax.broadcasted_iota(jnp.int32, (rows, 1), 0) % TILE < TILE // 2
    for tile in range(3):
        spot = lax.broadcasted_iota(jnp.int32, (rows, pairs), 0)
        if tile == 2:
            spot = spot - spot % TILE + spot % (TILE // 2)
        pick = (spot + tile * rows == slots).astype(jnp.float32)
        pick_tok = (pick[:, :tokens] + pick[:, tokens:]).astype(BF)
        acts = contract(pick_tok, act_ref[...], ((1,), (0,))).astype(BF)
        grads = contract(pick.astype(BF), grad_ref[...], ((1,), (0,))).astype(BF)
        if tile == 2:
            acts = jnp.where(lower, acts[:, :quarter], acts[:, quarter:])
        start = tile * width
        middle = start + acts.shape[1]
        for p in range(chips):
            out_ref[p, 0, :, start:middle] = acts[p * TILE : (p + 1) * TILE]
            out_ref[p, 0, :, middle : middle + grads.shape[1]] = grads[p * TILE : (p + 1) * TILE]


def fill(ids, act, grad, chips):
    tokens, features = act.shape
    pairs, hidden = grad.shape
    half = features // 2
    width = 2 * (half + hidden) + half // 2 + hidden
    return pl.pallas_call(
        functools.partial(fill_kernel, half),
        grid=(2,),
        in_specs=[
            pl.BlockSpec((2, tokens), lambda c: (0, 0)),
            pl.BlockSpec((tokens, half), lambda c: (0, c)),
            pl.BlockSpec((pairs, hidden), lambda c: (0, 0)),
        ],
        out_specs=pl.BlockSpec((chips, 1, TILE, width), lambda c: (0, c, 0, 0)),
        out_shape=jax.ShapeDtypeStruct((chips, 2, TILE, width), BF),
        cost_estimate=pl.CostEstimate(flops=2_000_000_000, bytes_accessed=6_000_000, transcendentals=0),
        name="fill_b",
    )(ids, act, grad)


def products_kernel(half, hidden, in_ref, out_ref):
    count = in_ref.shape[0] * TILE
    quarter = half // 2
    width = half + hidden

    def rows(start, size):
        return in_ref[:, :, start : start + size].reshape(count, size)

    row = lax.broadcasted_iota(jnp.int32, (count, 1), 0) % TILE
    for pair in range(2):
        for k in range(2):

            @pl.when((pl.program_id(0) == pair) & (pl.program_id(1) == k))
            def _():
                owner = row // 2 == pair * 2 + k
                last = jnp.where(owner, rows(2 * width + quarter, hidden), jnp.zeros((), BF))
                total = contract(rows(k * width + pair * quarter, quarter), rows(k * width + half, hidden), ((0,), (0,)))
                total = total + contract(rows(2 * width, quarter), last, ((0,), (0,)))
                out_ref[...] = total.astype(BF).reshape(out_ref.shape)


def products(recv, half, hidden):
    block = half // 4
    return pl.pallas_call(
        functools.partial(products_kernel, half, hidden),
        grid=(2, 2),
        in_specs=[pl.BlockSpec(recv.shape, lambda r, k: (0, 0, 0))],
        out_specs=pl.BlockSpec((2, 1, block, hidden), lambda r, k: (r, k, 0, 0)),
        out_shape=jax.ShapeDtypeStruct((4, 2, block, hidden), BF),
        cost_estimate=pl.CostEstimate(flops=4_000_000_000, bytes_accessed=12_000_000, transcendentals=0),
        name="products_b",
    )(recv)


def sort_acts_kernel(spots, most, meta_ref, *refs):
    blocks, rows_ref, slots_ref, held = refs[:8], refs[8], refs[9], refs[10]
    tokens = slots_ref.shape[1] // 2
    base = pl.program_id(0) * rows_ref.shape[0]
    row = lax.broadcasted_iota(jnp.int32, (rows_ref.shape[0], tokens), 0) + base
    picks = []
    for n, block in enumerate(blocks):
        told = block[tokens : tokens + 8, :tokens].astype(jnp.float32).astype(jnp.int32)
        pick = None
        for k in range(2):
            expert, pos = told[2 * k : 2 * k + 1], told[2 * k + 1 : 2 * k + 2]
            slot = (expert % spots) * (8 * most) + meta_ref[n] * most + pos
            slot = jnp.where(expert // spots == meta_ref[8], slot, -1)
            slots_ref[n : n + 1, k * tokens : (k + 1) * tokens] = slot
            hit = row == slot
            pick = hit if pick is None else pick | hit
        picks.append(pick.astype(BF))

    @pl.when(pl.program_id(0) == 0)
    def _():
        for n, block in enumerate(blocks):
            held[n * tokens : (n + 1) * tokens, :] = block[:tokens, :]

    rows_ref[...] = contract(jnp.concatenate(picks, axis=1), held[...], ((1,), (0,))).astype(BF)


def sort_acts(blocks, meta, tokens, spots, most):
    width = blocks[0].shape[1]
    total = spots * 8 * most
    return pl.pallas_call(
        functools.partial(sort_acts_kernel, spots, most),
        grid=(2,),
        in_specs=[pl.BlockSpec(memory_space=pltpu.SMEM)] + [pl.BlockSpec(b.shape, lambda i: (0, 0)) for b in blocks],
        out_specs=[pl.BlockSpec((total // 2, width), lambda i: (i, 0)), pl.BlockSpec((8, 2 * tokens), lambda i: (0, 0))],
        out_shape=[jax.ShapeDtypeStruct((total, width), BF), jax.ShapeDtypeStruct((8, 2 * tokens), jnp.int32)],
        scratch_shapes=[pltpu.VMEM((8 * tokens, width), BF)],
        cost_estimate=pl.CostEstimate(flops=2_400_000_000, bytes_accessed=5_000_000, transcendentals=0),
        name="sort_acts",
    )(meta, *blocks)


def sort_grads_kernel(at_ref, slots_ref, *refs):
    parts, rows_ref, held = refs[:-2], refs[-2], refs[-1]
    pairs = slots_ref.shape[1]
    base = pl.program_id(0) * rows_ref.shape[0]
    row = lax.broadcasted_iota(jnp.int32, (rows_ref.shape[0], pairs), 0) + base

    @pl.when(pl.program_id(0) == 0)
    def _():
        start = 0
        for part in parts:
            held[start : start + part.shape[0], :] = part[...]
            start += part.shape[0]

    picks = [(row == slots_ref[pl.ds(at_ref[n], 1), :]).astype(BF) for n in range(8)]
    rows_ref[...] = contract(jnp.concatenate(picks, axis=1), held[...], ((1,), (0,))).astype(BF)


def sort_grads(parts, slots, at, total):
    width = parts[0].shape[1]
    pairs = slots.shape[1]
    return pl.pallas_call(
        sort_grads_kernel,
        grid=(2,),
        in_specs=[pl.BlockSpec(memory_space=pltpu.SMEM), pl.BlockSpec(slots.shape, lambda i: (0, 0))]
        + [pl.BlockSpec(p.shape, lambda i: (0, 0)) for p in parts],
        out_specs=pl.BlockSpec((total // 2, width), lambda i: (i, 0)),
        out_shape=jax.ShapeDtypeStruct((total, width), BF),
        scratch_shapes=[pltpu.VMEM((8 * pairs, width), BF)],
        cost_estimate=pl.CostEstimate(flops=5_400_000_000, bytes_accessed=7_000_000, transcendentals=0),
        name="sort_grads",
    )(at, slots, *parts)


def ordered(block_in, target):
    planes = lax.axis_size(Z)
    return lax.ppermute(block_in, Z, [(z, target(z) % planes) for z in range(planes)])


def shards(act_a, grad_a, route_a, act_b, grad_b, route_b):
    tokens, top = route_a.shape
    pairs = tokens * top
    features = act_a.shape[1]
    hidden = grad_a.shape[2]
    planes = lax.axis_size(Z)
    spots = lax.axis_size(PLANE)
    chips = spots // 2
    most = 5
    quarter = features // 4
    half = features // 2
    my_zh = lax.axis_index("zh")
    my_zl = lax.axis_index("zl")
    my_z = 2 * my_zh + my_zl
    sign = 1 - 2 * my_zl

    grads = jnp.moveaxis(grad_a, 1, 0).reshape(pairs, hidden)
    up, down = [grads], [grads]
    for _ in range(1, 4):
        up.append(ordered(up[-1], lambda z: z + 1))
        down.append(ordered(down[-1], lambda z: z - 1))
    across = [ordered(up[3][:tokens], lambda z: z + 1), ordered(down[3][tokens:], lambda z: z - 1)]
    ring = (0, -1, -2, -3, 4, 3, 2, 1)

    ids_a = route_a.T
    pos_a = positions(ids_a.reshape(-1)).reshape(top, tokens)
    info = jnp.stack([ids_a, pos_a], axis=1).reshape(2 * top, tokens).astype(BF)
    info = jnp.pad(info, ((0, 8 - 2 * top), (0, quarter - tokens)))
    quarters = jnp.moveaxis(act_a.reshape(tokens, 4, quarter), 1, 0)

    def mine(which):
        rows = lax.dynamic_index_in_dim(quarters, lax.rem(which + 8, 4), 0, keepdims=False)
        return jnp.concatenate([rows, info], axis=0)

    def along(block_in, step):
        return ordered(block_in, lambda z: z + step * (1 - 2 * (z % 2)))

    near = [mine(my_zh)]
    for to, step in ((my_zh + 2, -3), (my_zh + sign, 2), (my_zh - sign, -1)):
        near.append(along(mine(to), step))
    offsets = (0, -3, -2, -1, 1, 4, 3, 2)
    far = [along(b, 1) for b in near]

    grads_b = jnp.moveaxis(grad_b, 1, 0).reshape(pairs, hidden)
    send_b = fill(route_b.T, act_b, grads_b, chips)
    recv_b = lax.all_to_all(send_b.reshape(spots, TILE, send_b.shape[-1]), PLANE, 0, 0, tiled=True)

    parts = products(recv_b, half, hidden).reshape(features, hidden)
    wgrad_b = lax.psum_scatter(parts, Z, scatter_dimension=0, tiled=True)[None]

    total = spots * planes * most
    origin = [lax.rem(my_z + o * sign + planes, planes) for o in offsets]
    rows_a, slots = sort_acts(near + far, jnp.stack(origin + [my_zl]), tokens, spots, most)
    even = [offsets.index(o) for o in ring]
    odd = [offsets.index(-o if -o in offsets else 4) for o in ring]
    at = jnp.stack([jnp.where(my_zl == 0, e, o).astype(jnp.int32) for e, o in zip(even, odd)])
    rows_g = sort_grads(up + across + down[:0:-1], slots, at, total)
    rows_a = rows_a.reshape(spots, planes * most, quarter)
    rows_g = rows_g.reshape(spots, planes * most, hidden)
    recv_a = lax.all_to_all(rows_a, PLANE, 0, 0, tiled=True).reshape(total, quarter)
    recv_g = lax.all_to_all(rows_g, PLANE, 0, 0, tiled=True).reshape(total, hidden)
    wgrad_a = contract(recv_a, recv_g, ((0,), (0,))).astype(BF)[None]
    return wgrad_a, wgrad_b


def solution(mesh):
    fine = Mesh(mesh.devices.reshape(4, 2, 4, 4, 2), ALL)
    return jax.shard_map(
        shards,
        mesh=fine,
        in_specs=tuple(P(ALL, *([None] * n)) for n in (1, 2, 1, 1, 2, 1)),
        out_specs=(P(("zl",) + PLANE, "zh", None),) * 2,
        check_vma=False,
    )
```

```python
import functools

import jax
import jax.numpy as jnp
from jax import lax
from jax.experimental import pallas as pl
from jax.experimental.pallas import tpu as pltpu
from jax.sharding import Mesh, PartitionSpec as P

Z = ("zh", "zl")
PLANE = ("x", "y", "c")
ALL = Z + PLANE
BF = jnp.bfloat16
TILE = 8


def contract(left, right, dims):
    return lax.dot_general(left, right, (dims, ((), ())), preferred_element_type=jnp.float32)


def positions(ids):
    order = jnp.arange(ids.shape[0], dtype=jnp.int32)
    same = (ids[:, None] == ids[None, :]) & (order[:, None] < order[None, :])
    return jnp.sum(same.astype(jnp.int32), axis=0)


def fill_kernel(half, ids_ref, act_ref, grad_ref, out_ref):
    chips = out_ref.shape[0]
    rows = chips * TILE
    tokens = ids_ref.shape[1]
    pairs = 2 * tokens
    width = half + grad_ref.shape[1]
    quarter = half // 2
    ids = jnp.concatenate([ids_ref[0:1, :], ids_ref[1:2, :]], axis=1)
    named = (lax.broadcasted_iota(jnp.int32, (2 * chips, pairs), 0) == ids).astype(jnp.float32)
    earlier = lax.broadcasted_iota(jnp.int32, (pairs, pairs), 0) < lax.broadcasted_iota(jnp.int32, (pairs, pairs), 1)
    before = contract(named.astype(BF), earlier.astype(BF), ((1,), (0,)))
    pos = jnp.sum(named * before, axis=0, keepdims=True).astype(jnp.int32)
    expert = ids // chips
    row = jnp.where(pos < TILE, expert * rows + pos, 2 * rows + expert * 2 + pos - TILE)
    slots = (ids % chips) * TILE + row
    lower = lax.broadcasted_iota(jnp.int32, (rows, 1), 0) % TILE < TILE // 2
    for tile in range(3):
        spot = lax.broadcasted_iota(jnp.int32, (rows, pairs), 0)
        if tile == 2:
            spot = spot - spot % TILE + spot % (TILE // 2)
        pick = (spot + tile * rows == slots).astype(jnp.float32)
        pick_tok = (pick[:, :tokens] + pick[:, tokens:]).astype(BF)
        acts = contract(pick_tok, act_ref[...], ((1,), (0,))).astype(BF)
        grads = contract(pick.astype(BF), grad_ref[...], ((1,), (0,))).astype(BF)
        if tile == 2:
            acts = jnp.where(lower, acts[:, :quarter], acts[:, quarter:])
            grads = jnp.where(lower, grads[:, : grads.shape[1] // 2], grads[:, grads.shape[1] // 2 :])
        start = tile * width
        middle = start + acts.shape[1]
        for p in range(chips):
            out_ref[p, 0, :, start:middle] = acts[p * TILE : (p + 1) * TILE]
            out_ref[p, 0, :, middle : middle + grads.shape[1]] = grads[p * TILE : (p + 1) * TILE]


def fill(ids, act, grad, chips):
    tokens, features = act.shape
    pairs, hidden = grad.shape
    half = features // 2
    width = 2 * (half + hidden) + (half + hidden) // 2
    return pl.pallas_call(
        functools.partial(fill_kernel, half),
        grid=(2,),
        in_specs=[
            pl.BlockSpec((2, tokens), lambda c: (0, 0)),
            pl.BlockSpec((tokens, half), lambda c: (0, c)),
            pl.BlockSpec((pairs, hidden), lambda c: (0, 0)),
        ],
        out_specs=pl.BlockSpec((chips, 1, TILE, width), lambda c: (0, c, 0, 0)),
        out_shape=jax.ShapeDtypeStruct((chips, 2, TILE, width), BF),
        cost_estimate=pl.CostEstimate(flops=2_000_000_000, bytes_accessed=6_000_000, transcendentals=0),
        name="fill_b",
    )(ids, act, grad)


def products_kernel(half, hidden, in_ref, out_ref):
    count = in_ref.shape[0] * TILE
    quarter = half // 2
    width = half + hidden

    def rows(start, size):
        return in_ref[:, :, start : start + size].reshape(count, size)

    row = lax.broadcasted_iota(jnp.int32, (count, 1), 0) % TILE
    for pair in range(2):
        for k in range(2):

            @pl.when((pl.program_id(0) == pair) & (pl.program_id(1) == k))
            def _():
                owner = row // 2 == pair * 2 + k
                near = rows(2 * width + quarter, hidden // 2).astype(jnp.float32)
                if pair == 0:
                    ends = [near, pltpu.roll(near, count - TILE // 2, 0)]
                else:
                    ends = [pltpu.roll(near, TILE // 2, 0), near]
                last = jnp.where(owner, jnp.concatenate(ends, axis=1), 0.0).astype(BF)
                total = contract(rows(k * width + pair * quarter, quarter), rows(k * width + half, hidden), ((0,), (0,)))
                total = total + contract(rows(2 * width, quarter), last, ((0,), (0,)))
                out_ref[...] = total.astype(BF).reshape(out_ref.shape)


def products(recv, half, hidden):
    block = half // 4
    return pl.pallas_call(
        functools.partial(products_kernel, half, hidden),
        grid=(2, 2),
        in_specs=[pl.BlockSpec(recv.shape, lambda r, k: (0, 0, 0))],
        out_specs=pl.BlockSpec((2, 1, block, hidden), lambda r, k: (r, k, 0, 0)),
        out_shape=jax.ShapeDtypeStruct((4, 2, block, hidden), BF),
        cost_estimate=pl.CostEstimate(flops=4_000_000_000, bytes_accessed=12_000_000, transcendentals=0),
        name="products_b",
    )(recv)


def sort_acts_kernel(spots, most, meta_ref, *refs):
    blocks, rows_ref, slots_ref, held = refs[:8], refs[8], refs[9], refs[10]
    tokens = slots_ref.shape[1] // 2
    base = pl.program_id(0) * rows_ref.shape[0]
    row = lax.broadcasted_iota(jnp.int32, (rows_ref.shape[0], tokens), 0) + base
    picks = []
    for n, block in enumerate(blocks):
        told = block[tokens : tokens + 8, :tokens].astype(jnp.float32).astype(jnp.int32)
        pick = None
        for k in range(2):
            expert, pos = told[2 * k : 2 * k + 1], told[2 * k + 1 : 2 * k + 2]
            slot = (expert % spots) * (8 * most) + meta_ref[n] * most + pos
            slot = jnp.where(expert // spots == meta_ref[8], slot, -1)
            slots_ref[n : n + 1, k * tokens : (k + 1) * tokens] = slot
            hit = row == slot
            pick = hit if pick is None else pick | hit
        picks.append(pick.astype(BF))

    @pl.when(pl.program_id(0) == 0)
    def _():
        for n, block in enumerate(blocks):
            held[n * tokens : (n + 1) * tokens, :] = block[:tokens, :]

    rows_ref[...] = contract(jnp.concatenate(picks, axis=1), held[...], ((1,), (0,))).astype(BF)


def sort_acts(blocks, meta, tokens, spots, most):
    width = blocks[0].shape[1]
    total = spots * 8 * most
    return pl.pallas_call(
        functools.partial(sort_acts_kernel, spots, most),
        grid=(2,),
        in_specs=[pl.BlockSpec(memory_space=pltpu.SMEM)] + [pl.BlockSpec(b.shape, lambda i: (0, 0)) for b in blocks],
        out_specs=[pl.BlockSpec((total // 2, width), lambda i: (i, 0)), pl.BlockSpec((8, 2 * tokens), lambda i: (0, 0))],
        out_shape=[jax.ShapeDtypeStruct((total, width), BF), jax.ShapeDtypeStruct((8, 2 * tokens), jnp.int32)],
        scratch_shapes=[pltpu.VMEM((8 * tokens, width), BF)],
        cost_estimate=pl.CostEstimate(flops=2_400_000_000, bytes_accessed=5_000_000, transcendentals=0),
        name="sort_acts",
    )(meta, *blocks)


def sort_grads_kernel(at_ref, slots_ref, *refs):
    parts, rows_ref, held = refs[:-2], refs[-2], refs[-1]
    pairs = slots_ref.shape[1]
    base = pl.program_id(0) * rows_ref.shape[0]
    row = lax.broadcasted_iota(jnp.int32, (rows_ref.shape[0], pairs), 0) + base

    @pl.when(pl.program_id(0) == 0)
    def _():
        start = 0
        for part in parts:
            held[start : start + part.shape[0], :] = part[...]
            start += part.shape[0]

    picks = [(row == slots_ref[pl.ds(at_ref[n], 1), :]).astype(BF) for n in range(8)]
    rows_ref[...] = contract(jnp.concatenate(picks, axis=1), held[...], ((1,), (0,))).astype(BF)


def sort_grads(parts, slots, at, total):
    width = parts[0].shape[1]
    pairs = slots.shape[1]
    return pl.pallas_call(
        sort_grads_kernel,
        grid=(2,),
        in_specs=[pl.BlockSpec(memory_space=pltpu.SMEM), pl.BlockSpec(slots.shape, lambda i: (0, 0))]
        + [pl.BlockSpec(p.shape, lambda i: (0, 0)) for p in parts],
        out_specs=pl.BlockSpec((total // 2, width), lambda i: (i, 0)),
        out_shape=jax.ShapeDtypeStruct((total, width), BF),
        scratch_shapes=[pltpu.VMEM((8 * pairs, width), BF)],
        cost_estimate=pl.CostEstimate(flops=5_400_000_000, bytes_accessed=7_000_000, transcendentals=0),
        name="sort_grads",
    )(at, slots, *parts)


def ordered(block_in, target):
    planes = lax.axis_size(Z)
    return lax.ppermute(block_in, Z, [(z, target(z) % planes) for z in range(planes)])


def shards(act_a, grad_a, route_a, act_b, grad_b, route_b):
    tokens, top = route_a.shape
    pairs = tokens * top
    features = act_a.shape[1]
    hidden = grad_a.shape[2]
    planes = lax.axis_size(Z)
    spots = lax.axis_size(PLANE)
    chips = spots // 2
    most = 5
    quarter = features // 4
    half = features // 2
    my_zh = lax.axis_index("zh")
    my_zl = lax.axis_index("zl")
    my_z = 2 * my_zh + my_zl
    sign = 1 - 2 * my_zl

    grads = jnp.moveaxis(grad_a, 1, 0).reshape(pairs, hidden)
    up, down = [grads], [grads]
    for _ in range(1, 4):
        up.append(ordered(up[-1], lambda z: z + 1))
        down.append(ordered(down[-1], lambda z: z - 1))
    across = [ordered(up[3][:tokens], lambda z: z + 1), ordered(down[3][tokens:], lambda z: z - 1)]
    ring = (0, -1, -2, -3, 4, 3, 2, 1)

    ids_a = route_a.T
    pos_a = positions(ids_a.reshape(-1)).reshape(top, tokens)
    info = jnp.stack([ids_a, pos_a], axis=1).reshape(2 * top, tokens).astype(BF)
    info = jnp.pad(info, ((0, 8 - 2 * top), (0, quarter - tokens)))
    quarters = jnp.moveaxis(act_a.reshape(tokens, 4, quarter), 1, 0)

    def mine(which):
        rows = lax.dynamic_index_in_dim(quarters, lax.rem(which + 8, 4), 0, keepdims=False)
        return jnp.concatenate([rows, info], axis=0)

    def along(block_in, step):
        return ordered(block_in, lambda z: z + step * (1 - 2 * (z % 2)))

    near = [mine(my_zh)]
    for to, step in ((my_zh + 2, -3), (my_zh + sign, 2), (my_zh - sign, -1)):
        near.append(along(mine(to), step))
    offsets = (0, -3, -2, -1, 1, 4, 3, 2)
    far = [along(b, 1) for b in near]

    grads_b = jnp.moveaxis(grad_b, 1, 0).reshape(pairs, hidden)
    send_b = fill(route_b.T, act_b, grads_b, chips)
    recv_b = lax.all_to_all(send_b.reshape(spots, TILE, send_b.shape[-1]), PLANE, 0, 0, tiled=True)

    parts = products(recv_b, half, hidden).reshape(features, hidden)
    wgrad_b = lax.psum_scatter(parts, Z, scatter_dimension=0, tiled=True)[None]

    total = spots * planes * most
    origin = [lax.rem(my_z + o * sign + planes, planes) for o in offsets]
    rows_a, slots = sort_acts(near + far, jnp.stack(origin + [my_zl]), tokens, spots, most)
    even = [offsets.index(o) for o in ring]
    odd = [offsets.index(-o if -o in offsets else 4) for o in ring]
    at = jnp.stack([jnp.where(my_zl == 0, e, o).astype(jnp.int32) for e, o in zip(even, odd)])
    rows_g = sort_grads(up + across + down[:0:-1], slots, at, total)
    rows_a = rows_a.reshape(spots, planes * most, quarter)
    rows_g = rows_g.reshape(spots, planes * most, hidden)
    recv_a = lax.all_to_all(rows_a, PLANE, 0, 0, tiled=True).reshape(total, quarter)
    recv_g = lax.all_to_all(rows_g, PLANE, 0, 0, tiled=True).reshape(total, hidden)
    wgrad_a = contract(recv_a, recv_g, ((0,), (0,))).astype(BF)[None]
    return wgrad_a, wgrad_b


def solution(mesh):
    fine = Mesh(mesh.devices.reshape(4, 2, 4, 4, 2), ALL)
    return jax.shard_map(
        shards,
        mesh=fine,
        in_specs=tuple(P(ALL, *([None] * n)) for n in (1, 2, 1, 1, 2, 1)),
        out_specs=(P(("zl",) + PLANE, "zh", None),) * 2,
        check_vma=False,
    )
```
